16 devices in a mesh: rep: 1, dp: 16 (over x, y, z, core).
Axes of the slice: x: 2, y: 2, z: 2, core: 2. Of those that a mesh axis runs over, the one named last changes fastest.
Arguments:
- x: bfloat16 [16, 2048, 1280], P(('rep', 'dp'))
- dy: bfloat16 [16, 2048, 1280], P(('rep', 'dp'))
- w_gate: bfloat16 [2, 1280, 4480], P(None, 'dp')
- w_up: bfloat16 [2, 1280, 4480], P(None, 'dp')
- w_down: bfloat16 [2, 4480, 1280], P(None, 'dp')
Outputs:
- output 1: bfloat16 [16, 2048, 1280], P(('rep', 'dp'))
- output 2: bfloat16 [2, 1280, 4480], P('rep', 'dp')
- output 3: bfloat16 [2, 1280, 4480], P('rep', 'dp')
- output 4: bfloat16 [2, 4480, 1280], P('rep', 'dp')
All inputs are finite; a program needn't handle non-finite values.
Results may differ from the reference program's by a relative error of at most 0.018.
Values are sent between devices in bfloat16 or wider.
A program may use at most 2 GiB of HBM per device.

```python
import jax
import jax.numpy as jnp
from jax import lax

SEQUENCES = 16
TOKENS = 2048
D = 1280
FF = 4480
LAYERS = 2
NAMES = ("w_gate", "w_up", "w_down")
SHAPES = {"w_gate": (LAYERS, D, FF), "w_up": (LAYERS, D, FF), "w_down": (LAYERS, FF, D)}


def bump(key, n, height):
    away = (jnp.arange(n, dtype=jnp.int32) - jax.random.randint(key, (), 0, n, jnp.int32)) % n
    return jnp.where(away < n // 8, height, 1.0)


def together(key, own, strength):
    shared = jax.random.normal(key, own.shape[1:], jnp.float32)
    return (own + strength * shared) * lax.rsqrt(1 + strength * strength)


def setup_inputs(seed: int = 0, part: int = 0) -> dict:
    kx, kdy, ka, kb, kz, kf, kh, kl, *kw = jax.random.split(jax.random.key(seed), 8 + len(NAMES))
    kx, kdy, ka, kb = (jax.random.fold_in(k, part) for k in (kx, kdy, ka, kb))
    shape = (SEQUENCES, TOKENS, D)
    much_x, much_dy = jax.random.uniform(kz, (2,), jnp.float32, 0.0, 1.0)
    layers = 2.0 ** jax.random.uniform(kl, (LAYERS, 1, 1), jnp.float32, -1.0, 1.0)
    x = together(ka, jax.random.normal(kx, shape, jnp.float32), much_x) * bump(kf, D, 4.0)
    dy = together(kb, jax.random.normal(kdy, shape, jnp.float32), much_dy)
    drawn = {"x": x.astype(jnp.bfloat16), "dy": (dy * (SEQUENCES * TOKENS) ** -0.5).astype(jnp.bfloat16)}
    for key, name in zip(kw, NAMES, strict=True):
        w = jax.random.normal(key, SHAPES[name], jnp.float32) * SHAPES[name][1] ** -0.5
        drawn[name] = (w * {"w_gate": 1.0, "w_up": bump(kh, FF, 4.0), "w_down": layers}[name]).astype(jnp.bfloat16)
    return drawn


def matmul(a, w):
    return jnp.dot(a, w, preferred_element_type=jnp.float32).astype(jnp.bfloat16)


def normed(h):
    wide = h.astype(jnp.float32)
    scale = lax.rsqrt(jnp.mean(wide**2, -1, keepdims=True) + 1e-6)
    return (wide * scale).astype(jnp.bfloat16)


def layer(h, w):
    a = normed(h)
    gate = jnp.dot(a, w["w_gate"], preferred_element_type=jnp.float32)
    up = jnp.dot(a, w["w_up"], preferred_element_type=jnp.float32)
    return h + matmul((jax.nn.silu(gate) * up).astype(jnp.bfloat16), w["w_down"])


def stack(weights, h):
    return lax.scan(lambda h, w: (layer(h, w), None), h, weights)[0]


def reference(x, dy, w_gate, w_up, w_down):
    weights = dict(zip(NAMES, (w_gate, w_up, w_down), strict=True))

    def take(so_far, sequence):
        h, by_y = sequence
        _, back = jax.vjp(stack, weights, h)
        by_weights, by_h = back(by_y)
        return jax.tree.map(lambda total, term: total + term.astype(jnp.float32), so_far, by_weights), by_h

    none_yet = {name: jnp.zeros(w.shape, jnp.float32) for name, w in weights.items()}
    by_weights, by_x = lax.scan(take, none_yet, (x, dy))
    return (by_x, *(by_weights[name].astype(jnp.bfloat16) for name in NAMES))
```

```python
import jax
import jax.numpy as jnp
from jax import lax
from jax.experimental import pallas as pl
from jax.experimental.pallas import tpu as pltpu
from jax.sharding import PartitionSpec as P

EPS = 1e-6
BF = jnp.bfloat16
F32 = jnp.float32
MESH = pl.DeviceIdType.MESH
ORDERS = ((0, 1, 2), (1, 2, 0), (2, 0, 1))
LAGS = (1, 3, 5, 6)


def gather_all(shards):
    parts = []
    for i, s in enumerate(shards):
        step = 512 if s.shape[1] > s.shape[0] * 16 else 256
        parts += [(i, c0, min(step, s.shape[1] - c0)) for c0 in range(0, s.shape[1], step)]
    n, total = len(shards), len(parts)

    def kernel(*refs):
        srcs, dsts, stage = refs[:n], refs[n : 2 * n], refs[2 * n : 3 * n]
        local, sent, got = refs[3 * n :]
        me = lax.axis_index("dp")
        core, xyz = me % 2, (me // 8, (me // 4) % 2, (me // 2) % 2)
        near = [me + 8 * (1 - 2 * xyz[0]), me + 4 * (1 - 2 * xyz[1]), me + 2 * (1 - 2 * xyz[2]), me + (1 - 2 * core)]
        whole = dsts
        ins = [pltpu.make_async_copy(srcs[i], stage[i], local.at[i]) for i in range(n)]
        for c in ins:
            c.start()
        barrier = pltpu.get_barrier_semaphore()
        for d in near:
            pl.semaphore_signal(barrier, inc=1, device_id={"dp": d}, device_id_type=MESH)
        for c in ins:
            c.wait()
        own = [pltpu.make_async_copy(stage[i], whole[i].at[(*xyz, core)], local.at[i]) for i in range(n)]
        for c in own:
            c.start()
        pl.semaphore_wait(barrier, 4)

        def hop(p, r):
            i, c0, width = parts[p]
            order = ORDERS[p % 3]
            at = list(xyz)
            for k in range(min(r, 3)):
                at[order[k]] = slice(None)
            there = whole[i].at[at[0], at[1], at[2], core, :, pl.ds(c0, width)]
            here = stage[i].at[:, pl.ds(c0, width)] if r == 0 else there
            return pltpu.make_async_remote_copy(
                here, there, sent.at[p, r], got.at[p, r],
                device_id={"dp": near[3] if r == 3 else near[order[r]]}, device_id_type=MESH)

        for t in range(total + LAGS[3] + 1):
            if t == LAGS[0]:
                for c in own:
                    c.wait()
            if t < total:
                hop(t, 0).start()
            for r in range(4):
                p = t - LAGS[r]
                if 0 <= p < total:
                    hop(p, r).wait_recv()
                    if r < 3:
                        hop(p, r + 1).start()
        for p in range(total):
            for r in range(4):
                hop(p, r).wait_send()

    made = pl.pallas_call(
        kernel,
        out_shape=[jax.ShapeDtypeStruct((2, 2, 2, 2, *s.shape), s.dtype) for s in shards],
        in_specs=[pl.BlockSpec(memory_space=pl.ANY)] * n,
        out_specs=[pl.BlockSpec(memory_space=pl.ANY)] * n,
        scratch_shapes=[pltpu.VMEM(s.shape, s.dtype) for s in shards]
        + [pltpu.SemaphoreType.DMA((n,)), pltpu.SemaphoreType.DMA((total, 4)), pltpu.SemaphoreType.DMA((total, 4))],
        compiler_params=pltpu.CompilerParams(collective_id=0, has_side_effects=True, vmem_limit_bytes=40 * 2**20),
        name="gather_all",
    )(*shards)
    return [t.reshape(-1, t.shape[-1]) for t in made]


def norm_stats(h):
    wide = h.astype(F32)
    scale = lax.rsqrt(jnp.mean(wide**2, -1, keepdims=True) + EPS)
    return wide, scale


def dot(a, b, dims):
    return lax.dot_general(a, b, (dims, ((), ())), preferred_element_type=F32)


def solution(mesh):
    def body(x, dy, wg, wu, wd):
        x, dy = x[0], dy[0]
        layers = wg.shape[0]
        whole = gather_all([w[i] for i in range(layers) for w in (wg, wu, wd)])
        g_w, u_w, d_w = whole[0::3], whole[1::3], whole[2::3]
        saved = []
        h = x
        for i in range(layers):
            wide, scale = norm_stats(h)
            a = (wide * scale).astype(BF)
            gate = dot(a, g_w[i], ((1,), (0,)))
            up = dot(a, u_w[i], ((1,), (0,)))
            act = (jax.nn.silu(gate) * up).astype(BF)
            saved.append((h, a, gate, up, act))
            if i < layers - 1:
                h = h + dot(act, d_w[i], ((1,), (0,))).astype(BF)
        ct = dy
        out_g, out_u, out_d = [None] * layers, [None] * layers, [None] * layers
        scatter = lambda t: lax.psum_scatter(t.astype(BF), "dp", scatter_dimension=0, tiled=True)
        for i in reversed(range(layers)):
            h, a, gate, up, act = saved[i]
            dact = dot(ct, d_w[i], ((1,), (1,))).astype(BF)
            out_d[i] = scatter(dot(act, ct, ((0,), (0,))))
            da32 = dact.astype(F32)
            sig = jax.nn.sigmoid(gate)
            silu = gate * sig
            dup = (da32 * silu).astype(BF)
            dgate = (da32 * up * (sig * (1 + gate * (1 - sig)))).astype(BF)
            out_g[i] = scatter(dot(a, dgate, ((0,), (0,))))
            out_u[i] = scatter(dot(a, dup, ((0,), (0,))))
            da = dot(dgate, g_w[i], ((1,), (1,))).astype(BF) + dot(dup, u_w[i], ((1,), (1,))).astype(BF)
            wide, scale = norm_stats(h)
            daw = da.astype(F32)
            inner = jnp.mean(daw * wide, -1, keepdims=True)
            dh = daw * scale - wide * (scale**3 * inner)
            ct = ct + dh.astype(BF)
        return (ct[None], jnp.stack(out_g), jnp.stack(out_u), jnp.stack(out_d))

    return jax.shard_map(
        body, mesh=mesh,
        in_specs=(P(("rep", "dp")), P(("rep", "dp")), P(None, "dp"), P(None, "dp"), P(None, "dp")),
        out_specs=(P(("rep", "dp")), P("rep", "dp"), P("rep", "dp"), P("rep", "dp")),
        check_vma=False)
```
